32 devices in a mesh: chan: 8 (over z, y), period: 4 (over x, core).
Axes of the slice: x: 2, y: 2, z: 4, core: 2. Of those that a mesh axis runs over, the one named last changes fastest.
Arguments:
- raw_strain: bfloat16 [4, 2048, 512], P('period', 'chan'), may hold values from -16 to 16
- bin_ids: int32 [3, 512, 64], P(None, 'chan'), may hold values from 0 to 31, as said below
- owner_map: int32 [16], replicated, may hold values from 0 to 7, as said below
Outputs:
- stacks: float32 [32, 32, 256], P('chan')
The draws below stay inside these ranges and needn't reach their ends.
Inputs may be any that keep to these rules, and one draw needn't show every extreme that they name: `bin_ids`: for channel c of block b = c // 64 and partner block b - d, the value is l * 8 + o: the pair lies in midpoint bin 2 * (b - 1) + l with l from 0 to 3, and in offset bin o below 8. `owner_map`: nondecreasing in the bin; bin m belongs to device m // 2 or m // 2 + 1; no device owns more than 4 bins and some device owns exactly 4.
All inputs are finite; a program needn't handle non-finite values.
Results may differ from the reference program's by a relative error of at most 0.0025.
Values may be sent and summed in bfloat16 or wider, within the bound.
A program may use at most 64 MiB of HBM per device.

```python
import math
import jax
import jax.numpy as jnp
from jax import lax

CH_DEV = 64
WIN = 256
NF = 128
NWIN = 8
MB_DEV = 2
NOFF = 8
NP = 32
SAMPLES = 2048
CHANNELS = 512
PERIODS = 4
NMB = 16
CAP = 4
SLOTS = 32
N_CHAN = 8


def draw_raw_strain(key, part):
    noise_key = jax.random.fold_in(key, 11)
    gain_key = jax.random.fold_in(key, 12)
    log_gain = jax.random.uniform(gain_key, (PERIODS, 1, CHANNELS), jnp.float32, math.log(0.5), math.log(4.0))
    channel_gain = jnp.exp(log_gain)
    values = jnp.clip(jax.random.normal(noise_key, (PERIODS, SAMPLES, CHANNELS), jnp.float32), -4.0, 4.0)
    return (values * channel_gain).astype(jnp.bfloat16)


def draw_bin_ids(key, part):
    spread = max(CH_DEV // 8, 1)
    jitter = jax.random.randint(jax.random.fold_in(key, 21), (CHANNELS,), -spread, spread + 1)
    row_index = jnp.arange(CHANNELS, dtype=jnp.int32)[:, None]
    column = jnp.arange(CH_DEV, dtype=jnp.int32)[None, :]
    block_index = row_index // CH_DEV
    position = row_index + jitter[:, None]
    bin_width = CH_DEV // MB_DEV
    result = []
    for offset in range(3):
        partner = (block_index - offset) * CH_DEV + column
        partner_pos = partner + jnp.take(jitter, jnp.mod(partner, CHANNELS))
        midpoint = jnp.floor_divide(position + partner_pos, 2)
        local_bin = jnp.clip(jnp.floor_divide(midpoint, bin_width) - MB_DEV * (block_index - 1), 0, 2 * MB_DEV - 1)
        offset_bin = jnp.clip(jnp.abs(position - partner_pos) * NOFF // (3 * CH_DEV), 0, NOFF - 1)
        result.append(local_bin * NOFF + offset_bin)
    return jnp.stack(result).astype(jnp.int32)


def draw_owner_map(key, part):
    natural = NMB // MB_DEV
    moved_bins = jax.random.randint(jax.random.fold_in(key, 31), (natural,), 0, MB_DEV + 1)
    chosen = jax.random.randint(jax.random.fold_in(key, 32), (), 1, natural - 2)
    first_moved = jax.random.randint(jax.random.fold_in(key, 33), (), 0, MB_DEV)
    natural_index = jnp.arange(natural, dtype=jnp.int32)
    moved_bins = jnp.where(natural_index == chosen, MB_DEV, moved_bins)
    moved_bins = jnp.where(natural_index == chosen + 1, 0, moved_bins)
    moved_bins = jnp.where(natural_index == natural - 1, 0, moved_bins)
    moved_bins = jnp.where(natural_index == 0, first_moved, moved_bins)
    bin_index = jnp.arange(NMB, dtype=jnp.int32)
    home_owner = bin_index // MB_DEV
    shifted = (bin_index % MB_DEV >= MB_DEV - jnp.take(moved_bins, home_owner)).astype(jnp.int32)
    return (home_owner + shifted).astype(jnp.int32)


def setup_inputs(seed: int = 0) -> dict:
    key_of = jax.random.split(jax.random.key(seed), 4)
    raw_strain = draw_raw_strain(jax.random.fold_in(key_of[3], 71), 0)
    bin_ids = draw_bin_ids(jax.random.fold_in(key_of[3], 71), 0)
    owner_map = draw_owner_map(jax.random.fold_in(key_of[3], 71), 0)
    return dict(raw_strain=raw_strain, bin_ids=bin_ids, owner_map=owner_map)


def dft_table():
    sample_at = jnp.arange(WIN, dtype=jnp.int32)[:, None]
    freq_at = jnp.arange(1, NF + 1, dtype=jnp.int32)[None, :]
    phase_angle = 2.0 * math.pi / WIN * jnp.mod(sample_at * freq_at, WIN).astype(jnp.float32)
    return jnp.concatenate([jnp.cos(phase_angle), -jnp.sin(phase_angle)], axis=1).astype(jnp.bfloat16)

def lag_table():
    freq_at = jnp.arange(1, NF + 1, dtype=jnp.int32)[:, None]
    lag_at = jnp.arange(WIN, dtype=jnp.int32)[None, :]
    phase_angle = 2.0 * math.pi / WIN * jnp.mod(freq_at * lag_at, WIN).astype(jnp.float32)
    return jnp.concatenate([jnp.cos(phase_angle), -jnp.sin(phase_angle)], axis=0)

def slant_tables():
    slow_at = (jnp.arange(NP, dtype=jnp.float32) - NP // 2) / (4.0 * NP)
    offset_at = (jnp.arange(NOFF, dtype=jnp.float32) + 0.5) * (3.0 * CH_DEV / NOFF)
    freq_at = jnp.arange(1, NF + 1, dtype=jnp.float32) * (2.0 * math.pi / WIN)
    phase_angle = slow_at[:, None, None] * offset_at[None, :, None] * freq_at[None, None, :]
    return (jnp.cos(phase_angle), jnp.sin(phase_angle))

def whiten(spectra):
    power_mean = lax.optimization_barrier(jnp.mean(spectra * spectra, axis=-2, keepdims=True))
    return (spectra / jnp.sqrt(power_mean + 1e-06)).astype(jnp.bfloat16)

def slant_lags(binned):
    cos_table, sin_table = slant_tables()
    highest = lax.Precision.HIGHEST
    real_part = binned[..., :NF]
    imag_part = binned[..., NF:]
    slant_real = jnp.einsum('mof,qof->mqf', real_part, cos_table, precision=highest) + jnp.einsum('mof,qof->mqf', imag_part, sin_table, precision=highest)
    slant_imag = jnp.einsum('mof,qof->mqf', imag_part, cos_table, precision=highest) - jnp.einsum('mof,qof->mqf', real_part, sin_table, precision=highest)
    slant_spec = jnp.concatenate([slant_real, slant_imag], axis=-1)
    return jnp.einsum('mqk,kt->mqt', slant_spec, lag_table(), precision=highest)

def normalize(total_trace):
    return total_trace / jnp.sqrt(lax.optimization_barrier(jnp.mean(total_trace * total_trace, axis=-1, keepdims=True)) + 1e-06)

def period_bins(raw_period, bin_ids, dft_weights):
    windows = raw_period.reshape(NWIN, WIN, CHANNELS).astype(jnp.float32)
    spectra = jnp.einsum('wtc,tk->wkc', windows, dft_weights.astype(jnp.float32))
    whitened = whiten(spectra)
    blocks = jnp.transpose(whitened.reshape(NWIN, 2 * NF, N_CHAN, CH_DEV), (2, 0, 1, 3))
    padded = jnp.concatenate([jnp.zeros((2, NWIN, 2 * NF, CH_DEV), jnp.bfloat16), blocks], axis=0)

    def add_block(running, block_index):
        own_block = lax.dynamic_index_in_dim(padded, (block_index + 2).astype(jnp.int32), 0, keepdims=False).astype(jnp.float32)
        own_real = own_block[:, :NF, :]
        own_imag = own_block[:, NF:, :]
        for offset in range(3):
            other_block = lax.dynamic_index_in_dim(padded, (block_index + 2 - offset).astype(jnp.int32), 0, keepdims=False).astype(jnp.float32)
            other_real = other_block[:, :NF, :]
            other_imag = other_block[:, NF:, :]
            cross_real = jnp.einsum('wfi,wfj->fij', own_real, other_real) + jnp.einsum('wfi,wfj->fij', own_imag, other_imag)
            cross_imag = jnp.einsum('wfi,wfj->fij', own_imag, other_real) - jnp.einsum('wfi,wfj->fij', own_real, other_imag)
            cross_spec = jnp.concatenate([cross_real, cross_imag], axis=0).astype(jnp.bfloat16)
            cross_spec = lax.optimization_barrier(cross_spec).astype(jnp.float32)
            pair_values = cross_spec.reshape(2 * NF, CH_DEV * CH_DEV).T
            pair_ids = lax.dynamic_slice_in_dim(bin_ids[offset], (block_index * CH_DEV).astype(jnp.int32), CH_DEV, 0).reshape(-1)
            global_ids = pair_ids + MB_DEV * NOFF * (block_index - 1)
            global_ids = jnp.where(global_ids < 0, NMB * NOFF, global_ids).astype(jnp.int32)
            running = running + jax.ops.segment_sum(pair_values, global_ids, num_segments=NMB * NOFF)
        return (running, None)
    start_sum = jnp.zeros((NMB * NOFF, 2 * NF), jnp.float32)
    running, unused = lax.scan(add_block, start_sum, jnp.arange(N_CHAN, dtype=jnp.int32))
    return running.reshape(NMB, NOFF, 2 * NF)

def reference(raw_strain, bin_ids, owner_map):
    dft_weights = dft_table()
    total_trace = jnp.zeros((NMB, NP, WIN), jnp.float32)
    for period in range(PERIODS):
        binned = period_bins(raw_strain[period], bin_ids, dft_weights)
        total_trace = total_trace + slant_lags(binned)
    normed = normalize(total_trace)
    owners_below = lax.optimization_barrier(jnp.sum((owner_map[None, :] < owner_map[:, None]).astype(jnp.int32), axis=1))
    slot_rows = (owner_map * CAP + jnp.arange(NMB, dtype=jnp.int32) - owners_below).astype(jnp.int32)
    return jnp.zeros((SLOTS, NP, WIN), jnp.float32).at[slot_rows].set(normed)
```

```python
import functools
import math

import jax
import jax.numpy as jnp
import numpy as np
from jax import lax
from jax.experimental import pallas as pl
from jax.experimental.pallas import tpu as pltpu
from jax.sharding import PartitionSpec as P

CH_DEV = 64
WIN = 256
NF = 128
MB_DEV = 2
NOFF = 8
NP = 32


def passed_along(shard, axis, by):
    count = lax.axis_size(axis)
    pairs = [(i, i + by) for i in range(count) if 0 <= i + by < count]
    return lax.ppermute(shard, axis, pairs)


def with_halo(shard, sides, width):
    for axis, dim in sides:
        count, length = (lax.axis_size(axis), shard.shape[dim])
        up = [(i, (i + 1) % count) for i in range(count - 1)]
        down = [(j, i) for i, j in up]
        last = lax.slice_in_dim(shard, length - width, length, axis=dim)
        initial = lax.slice_in_dim(shard, 0, width, axis=dim)
        before = lax.ppermute(last, axis, up)
        after = lax.ppermute(initial, axis, down)
        shard = jnp.concatenate([before, shard, after], axis=dim)
    return shard


def dft_table():
    sample_at = jnp.arange(WIN, dtype=jnp.int32)[:, None]
    freq_at = jnp.arange(1, NF + 1, dtype=jnp.int32)[None, :]
    phase_angle = 2.0 * math.pi / WIN * jnp.mod(sample_at * freq_at, WIN).astype(jnp.float32)
    return jnp.concatenate([jnp.cos(phase_angle), -jnp.sin(phase_angle)], axis=1).astype(
        jnp.bfloat16
    )


def lag_table():
    freq_at = jnp.arange(1, NF + 1, dtype=jnp.int32)[:, None]
    lag_at = jnp.arange(WIN, dtype=jnp.int32)[None, :]
    phase_angle = 2.0 * math.pi / WIN * jnp.mod(freq_at * lag_at, WIN).astype(jnp.float32)
    return jnp.concatenate([jnp.cos(phase_angle), -jnp.sin(phase_angle)], axis=0)


def slant_tables():
    slow_at = (jnp.arange(NP, dtype=jnp.float32) - NP // 2) / (4.0 * NP)
    offset_at = (jnp.arange(NOFF, dtype=jnp.float32) + 0.5) * (3.0 * CH_DEV / NOFF)
    freq_at = jnp.arange(1, NF + 1, dtype=jnp.float32) * (2.0 * math.pi / WIN)
    phase_angle = slow_at[:, None, None] * offset_at[None, :, None] * freq_at[None, None, :]
    return (jnp.cos(phase_angle), jnp.sin(phase_angle))


def whiten_rows(spectra):
    power_mean = jnp.mean(spectra * spectra, axis=-1, keepdims=True)
    return (spectra / jnp.sqrt(power_mean + 1e-06)).astype(jnp.bfloat16)


def slant_lags(binned):
    cos_table, sin_table = slant_tables()
    highest = lax.Precision.HIGHEST
    real_part = binned[..., :NF]
    imag_part = binned[..., NF:]
    slant_real = jnp.einsum("mof,qof->mqf", real_part, cos_table, precision=highest) + jnp.einsum(
        "mof,qof->mqf", imag_part, sin_table, precision=highest
    )
    slant_imag = jnp.einsum("mof,qof->mqf", imag_part, cos_table, precision=highest) - jnp.einsum(
        "mof,qof->mqf", real_part, sin_table, precision=highest
    )
    slant_spec = jnp.concatenate([slant_real, slant_imag], axis=-1)
    return jnp.einsum("mqk,kt->mqt", slant_spec, lag_table(), precision=highest)


def normalize(total_trace):
    return total_trace / jnp.sqrt(
        jnp.mean(total_trace * total_trace, axis=-1, keepdims=True) + 1e-06
    )


def bin_pairs(own_spec, other_spec, pair_ids):
    freq_count = own_spec.shape[2] // 2
    channels = own_spec.shape[1]
    bin_count = 2 * MB_DEV * NOFF
    freq_block = min(32, freq_count)
    onehot = (
        lax.broadcasted_iota(jnp.int32, (bin_count, channels * channels), 0)
        == pair_ids.reshape(1, channels * channels)
    ).astype(jnp.bfloat16)
    real_cols = []
    imag_cols = []
    for freq_start in range(0, freq_count, freq_block):
        own_real = own_spec[:, :, freq_start : freq_start + freq_block]
        own_imag = own_spec[:, :, freq_count + freq_start : freq_count + freq_start + freq_block]
        other_real = other_spec[:, :, freq_start : freq_start + freq_block]
        other_imag = other_spec[
            :, :, freq_count + freq_start : freq_count + freq_start + freq_block
        ]
        left_side = jnp.stack(
            [
                jnp.concatenate([own_real, own_imag], axis=0),
                jnp.concatenate([own_imag, -own_real], axis=0),
            ]
        )
        right_side = jnp.concatenate([other_real, other_imag], axis=0)
        cross_block = jnp.einsum(
            "cwif,wjf->cfij", left_side, right_side, preferred_element_type=jnp.float32
        ).astype(jnp.bfloat16)
        flat_pairs = cross_block.reshape(2 * freq_block, channels * channels)
        binned_part = jnp.einsum(
            "np,rp->nr", onehot, flat_pairs, preferred_element_type=jnp.float32
        )
        real_cols.append(binned_part[:, :freq_block])
        imag_cols.append(binned_part[:, freq_block:])
    return jnp.concatenate(real_cols + imag_cols, axis=1)


def shards(raw_strain, bin_ids, owner_map):
    local_series = lax.all_to_all(raw_strain[0], "chan", split_axis=1, concat_axis=0, tiled=True)
    channels = local_series.shape[1]
    windows = local_series.reshape(local_series.shape[0] // WIN, WIN, channels)
    spectra = jnp.einsum("wtc,tk->wck", windows, dft_table(), preferred_element_type=jnp.float32)
    whitened = whiten_rows(spectra)
    near_spec = passed_along(whitened, "chan", 1)
    far_spec = passed_along(whitened, "chan", 2)
    partial_value = bin_pairs(whitened, whitened, bin_ids[0])
    partial_value = partial_value + bin_pairs(whitened, near_spec, bin_ids[1])
    partial_value = partial_value + bin_pairs(whitened, far_spec, bin_ids[2])
    beside_all = with_halo(partial_value[None], (("chan", 0),), 1)
    local_bins = 2 * MB_DEV
    capacity = 2 * MB_DEV
    device = lax.axis_index("chan")
    owned_count = jnp.sum((owner_map == device).astype(jnp.int32))
    first_bin = jnp.sum((owner_map < device).astype(jnp.int32))
    slot_at = lax.broadcasted_iota(jnp.int32, (capacity, 3, local_bins), 0)
    source_at = lax.broadcasted_iota(jnp.int32, (capacity, 3, local_bins), 1)
    place_at = lax.broadcasted_iota(jnp.int32, (capacity, 3, local_bins), 2)
    local_at = first_bin + slot_at - MB_DEV * (device + source_at - 2)
    select_rows = (
        ((local_at == place_at) & (slot_at < owned_count))
        .astype(jnp.float32)
        .reshape(capacity, 3 * local_bins)
    )
    stacked = beside_all.reshape(3 * local_bins, NOFF * 2 * NF)
    binned = jnp.dot(
        select_rows, stacked, precision=lax.Precision.HIGHEST, preferred_element_type=jnp.float32
    ).reshape(capacity, NOFF, 2 * NF)
    binned = lax.psum(binned, "period")
    total_trace = slant_lags(binned)
    return normalize(total_trace)


def host_tables():
    step = 2.0 * np.pi / WIN
    freq = np.arange(1, NF + 1)
    phase = step * np.mod(np.arange(WIN)[:, None] * freq[None, :], WIN)
    dft = np.concatenate([np.cos(phase), -np.sin(phase)], axis=1).astype(np.float32)
    lag = np.ascontiguousarray(dft_transposed(phase))
    slow = (np.arange(NP) - NP // 2) / (4.0 * NP)
    offset = (np.arange(NOFF) + 0.5) * (3.0 * CH_DEV / NOFF)
    angle = offset[:, None, None] * slow[None, :, None] * (freq * step)[None, None, :]
    return (
        dft.astype(jnp.bfloat16),
        lag,
        np.cos(angle).astype(np.float32),
        np.sin(angle).astype(np.float32),
    )


def dft_transposed(phase):
    return np.concatenate([np.cos(phase).T, -np.sin(phase).T], axis=0).astype(np.float32)


def flipped(me, by, count):
    result = 0
    bit = 1
    while bit < count:
        mine, other = (me // bit) % 2, (by // bit) % 2
        result = result + bit * (mine + other - 2 * mine * other)
        bit *= 2
    return result


GROUP = 64


def window_kernel(
    count, periods, bins, raw_hbm, ids_hbm, owner_hbm, dft_hbm, lag_hbm, cos_hbm, sin_hbm, out_ref,
    raw_ref, ids_ref, owner_ref, dft_ref, lag_ref, cos_ref, sin_ref, load_sem,
    id_buf, id_rows, spec, weights, part, part_send, part_recv, acc, total_buf,
    id_send, id_recv, raw_send, raw_recv, rs_send, rs_recv, ag_send, ag_recv,
):
    scope = jax.named_scope
    me = lax.axis_index("chan")
    period = lax.axis_index("period")
    side = lax.rem(period, 2)
    pair = period - side
    partner = pair + 1 - side
    blocks = count // 2
    width = (blocks + 2) * CH_DEV
    local = 2 * MB_DEV * NOFF
    step_rows = MB_DEV * NOFF
    half = CH_DEV // 2
    mesh_id = pl.DeviceIdType.MESH
    near = lax.div(me, blocks) == side
    mine = lax.rem(me, blocks)

    ids_load = pltpu.make_async_copy(ids_hbm, ids_ref, load_sem.at[0])
    ids_load.start()

    barrier = pltpu.get_barrier_semaphore()

    def greet(chan, to):
        pl.semaphore_signal(barrier, inc=1, device_id=(chan, to), device_id_type=mesh_id)

    for t in range(1, count):
        for s in range(2):
            greet(lax.rem(me + t, count), pair + s)
    greet(me, partner)
    for j in range(2, periods, 2):
        for s in range(2):
            greet(me, lax.rem(pair + j, periods) + s)

    def first_lane(which):
        return pl.multiple_of(which * ((blocks - 2) * CH_DEV), 2 * CH_DEV)

    loads = []
    for k, (source, target) in enumerate(
        (
            (raw_hbm.at[:, pl.ds(first_lane(side), width)], raw_ref.at[0]),
            (dft_hbm, dft_ref),
            (owner_hbm, owner_ref),
            (cos_hbm, cos_ref),
            (sin_hbm, sin_ref),
            (lag_hbm, lag_ref),
        )
    ):
        loads.append(pltpu.make_async_copy(source, target, load_sem.at[k + 1]))
        loads[-1].start()

    weights[0 : 2 * CH_DEV] = jnp.zeros((2 * CH_DEV, 4 * NF), jnp.bfloat16)
    part[...] = jnp.zeros_like(part)

    def id_copy(t, block):
        return pltpu.make_async_remote_copy(
            src_ref=id_buf.at[block],
            dst_ref=id_buf.at[block],
            send_sem=id_send.at[t],
            recv_sem=id_recv.at[block],
            device_id=(flipped(me, t, count), period),
            device_id_type=mesh_id,
        )

    raw_copy = pltpu.make_async_remote_copy(
        src_ref=raw_hbm.at[:, pl.ds(first_lane(1 - side), width)],
        dst_ref=raw_ref.at[1],
        send_sem=raw_send,
        recv_sem=raw_recv,
        device_id=(me, partner),
        device_id_type=mesh_id,
    )

    with scope("w_ids"):
        ids_load.wait()

    @pl.when(near)
    def _():
        close = jnp.concatenate([ids_ref[0], ids_ref[1]], axis=1)
        far = jnp.concatenate([ids_ref[2, :half], ids_ref[2, half:]], axis=1)
        id_buf[mine] = jnp.concatenate([close, far], axis=0).astype(jnp.float32).astype(jnp.bfloat16)

    with scope("w_barrier"):
        pl.semaphore_wait(barrier, 2 * (count - 1) + 1 + periods - 2)

    @pl.when(near)
    def _():
        for t in reversed(range(1, count)):
            id_copy(t, mine).start()

    raw_copy.start()

    def whiten_window(k):
        chunk = 2 * CH_DEV
        for start in range(0, width, chunk):
            spectra = lax.dot_general(
                raw_ref[k, :, start : start + chunk],
                dft_ref[...],
                (((0,), (0,)), ((), ())),
                preferred_element_type=jnp.float32,
            )
            whitened = whiten_rows(spectra)
            columns = slice(k * 2 * NF, (k + 1) * 2 * NF)
            weights[2 * CH_DEV + start : 2 * CH_DEV + start + chunk, columns] = whitened
            spec[start : start + chunk, columns] = whitened.astype(jnp.float32)

    loads[0].wait()
    loads[1].wait()
    whiten_window(0)
    with scope("w_raw"):
        raw_copy.wait_recv()
    whiten_window(1)

    bin_at = lax.broadcasted_iota(jnp.int32, (local, 4 * CH_DEV), 0).astype(jnp.float32)
    lane_at = lax.broadcasted_iota(jnp.int32, (half, 2 * CH_DEV), 1)

    def bin_block(block):
        ids = id_buf[block].astype(jnp.float32)
        id_rows[:, : 2 * CH_DEV] = ids[:CH_DEV]
        id_rows[:half, 2 * CH_DEV :] = jnp.where(lane_at < CH_DEV, ids[CH_DEV:], -1.0)
        id_rows[half:, 2 * CH_DEV :] = jnp.where(lane_at >= CH_DEV, ids[CH_DEV:], -1.0)
        own_block = block + 2 * side
        held = jnp.concatenate(
            [
                weights[pl.ds(pl.multiple_of((own_block + 2 - back) * CH_DEV, CH_DEV), CH_DEV)]
                for back in (0, 1, 2, 2)
            ],
            axis=0,
        )

        real = jnp.zeros((local, NF), jnp.float32)
        imag = jnp.zeros((local, NF), jnp.float32)
        for first in range(0, CH_DEV, GROUP):
            hot = []
            for u in range(GROUP):
                row = id_rows[first + u : first + u + 1, :]
                hot.append(jnp.where(row == bin_at, 1.0, 0.0).astype(jnp.bfloat16))
            summed = jnp.dot(
                jnp.concatenate(hot, axis=0), held, preferred_element_type=jnp.float32
            )
            for u in range(GROUP):
                own = spec[pl.ds(own_block * CH_DEV + first + u, 1), :]
                other = summed[u * local : (u + 1) * local]
                for k in range(2):
                    own_real = own[:, 2 * k * NF : (2 * k + 1) * NF]
                    own_imag = own[:, (2 * k + 1) * NF : (2 * k + 2) * NF]
                    other_real = other[:, 2 * k * NF : (2 * k + 1) * NF]
                    other_imag = other[:, (2 * k + 1) * NF : (2 * k + 2) * NF]
                    real = real + (own_real * other_real + own_imag * other_imag)
                    imag = imag + (own_imag * other_real - own_real * other_imag)
        rows = pl.ds(pl.multiple_of(block * step_rows, step_rows), local)
        part[rows, :NF] += real
        part[rows, NF:] += imag

    first_pair = side * blocks - 1

    def part_copy(k, upper):
        return pltpu.make_async_remote_copy(
            src_ref=part_send.at[k],
            dst_ref=part_recv.at[side, me],
            send_sem=rs_send.at[2 * k + upper],
            recv_sem=rs_recv.at[side, me],
            device_id=(first_pair + k + 1 - upper, pair + upper),
            device_id_type=mesh_id,
        )

    def goes(k, upper):
        owner = first_pair + k + 1 - upper
        elsewhere = jnp.logical_or(owner != me, side != upper)
        return (first_pair + k >= 0) & (owner < count) & elsewhere

    base = jnp.where(near, mine, lax.rem(me, 2) + (1 - side) * (blocks - 2))
    at_step = [flipped(base, block, blocks) for block in range(blocks)]
    done_at = [at_step[0]]
    done_at += [jnp.maximum(at_step[k - 1], at_step[k]) for k in range(1, blocks)]
    done_at += [at_step[blocks - 1]]

    def one_block(t, unused):
        block = flipped(base, t, blocks)

        @pl.when(jnp.logical_or(jnp.logical_not(near), t > 0))
        def _():
            with scope("w_id"):
                id_copy(1, block).wait_recv()

        with scope("bin"):
            bin_block(block)
        for k in range(blocks + 1):

            @pl.when(done_at[k] == t)
            def _():
                part_send[k] = part[k * step_rows : (k + 1) * step_rows].astype(part_send.dtype)
                for upper in range(2):

                    @pl.when(goes(k, upper))
                    def _():
                        part_copy(k, upper).start()

        return unused

    lax.fori_loop(0, blocks, one_block, 0)

    def part_arrival(from_side, source):
        return pltpu.make_async_remote_copy(
            src_ref=part_send.at[0],
            dst_ref=part_recv.at[from_side, source],
            send_sem=rs_send.at[0],
            recv_sem=rs_recv.at[from_side, source],
            device_id=(me, partner),
            device_id_type=mesh_id,
        )

    kept = me - 1 + side
    from_side = [
        (kept >= 0) & (kept < blocks),
        kept >= blocks - 1,
    ]
    from_own = jnp.where(side == 0, from_side[0], from_side[1])
    at = jnp.clip(kept - first_pair, 0, blocks)
    own_rows = part[pl.ds(pl.multiple_of(at * step_rows, step_rows), step_rows)]
    acc[...] = jnp.where(from_own, own_rows, 0.0)
    for s in range(2):

        @pl.when(from_side[s] & (side != s))
        def _():
            with scope("w_part"):
                part_arrival(s, me).wait_recv()
            acc[...] += part_recv[s, me].astype(jnp.float32)

        @pl.when(from_side[s])
        def _():
            total = acc[...]
            for t in range(1, count):
                source = flipped(me, t, count)
                with scope("w_part"):
                    part_arrival(s, source).wait_recv()
                total = total + part_recv[s, source].astype(jnp.float32)
            acc[...] = total

    total_buf[period] = acc[...].astype(total_buf.dtype)

    def total_copy(j, source):
        return pltpu.make_async_remote_copy(
            src_ref=total_buf.at[source],
            dst_ref=total_buf.at[source],
            send_sem=ag_send.at[j],
            recv_sem=ag_recv.at[source],
            device_id=(me, lax.rem(period + j, periods)),
            device_id_type=mesh_id,
        )

    for j in range(1, periods):
        total_copy(j, period).start()

    with scope("drain"):

        @pl.when(near)
        def _():
            for t in range(1, count):
                id_copy(t, mine).wait_send()

        raw_copy.wait_send()
        for k in range(blocks + 1):
            for upper in range(2):

                @pl.when(goes(k, upper))
                def _():
                    part_copy(k, upper).wait_send()

    for load in loads[2:]:
        load.wait()
    owned = jnp.int32(0)
    before = jnp.int32(0)
    for m in range(bins):
        owner = owner_ref[m]
        owned = owned + jnp.where(owner == me, 1, 0)
        before = before + jnp.where(owner < me, 1, 0)
    skipped = before - MB_DEV * (me - 1)

    with scope("w_total"):
        for j in range(1, periods):
            total_copy(j, lax.rem(period + periods - j, periods)).wait_recv()
    halves = []
    for s in range(2):
        total = total_buf[s].astype(jnp.float32)
        for p in range(s + 2, periods, 2):
            total = total + total_buf[p].astype(jnp.float32)
        halves.append(total)
    total = jnp.concatenate(halves, axis=0)

    capacity = 2 * MB_DEV
    slanted = []
    for slot in range(capacity):
        picked = jnp.zeros((NOFF, 2 * NF), jnp.float32)
        for c in range(2 * MB_DEV):
            wanted = jnp.where(slot < owned, skipped + slot, -1)
            picked = jnp.where(wanted == c, total[c * NOFF : (c + 1) * NOFF], picked)
        slant_real = jnp.zeros((NP, NF), jnp.float32)
        slant_imag = jnp.zeros((NP, NF), jnp.float32)
        for o in range(NOFF):
            real, imag = picked[o : o + 1, :NF], picked[o : o + 1, NF:]
            slant_real = slant_real + (real * cos_ref[o] + imag * sin_ref[o])
            slant_imag = slant_imag + (imag * cos_ref[o] - real * sin_ref[o])
        slanted.append(jnp.concatenate([slant_real, slant_imag], axis=1))
    traces = jnp.dot(
        jnp.concatenate(slanted, axis=0),
        lag_ref[...],
        precision=lax.Precision.HIGHEST,
        preferred_element_type=jnp.float32,
    )
    with scope("norm"):
        out_ref[...] = normalize(traces)
    for j in range(1, periods):
        total_copy(j, period).wait_send()


def window_shards(count, periods, raw_strain, bin_ids, owner_map):
    local = 2 * MB_DEV * NOFF
    step_rows = MB_DEV * NOFF
    blocks = count // 2
    width = (blocks + 2) * CH_DEV
    dft, lag, cos_table, sin_table = host_tables()
    dma = pltpu.SemaphoreType.DMA
    stacked = pl.pallas_call(
        functools.partial(window_kernel, count, periods, owner_map.shape[0]),
        out_shape=pltpu.VMEM((2 * MB_DEV * NP, WIN), jnp.float32),
        in_specs=[pl.BlockSpec(memory_space=pl.ANY)] * 7,
        out_specs=pl.BlockSpec(memory_space=pltpu.VMEM),
        scratch_shapes=[
            pltpu.VMEM((2, WIN, width), raw_strain.dtype),
            pltpu.VMEM(bin_ids.shape, bin_ids.dtype),
            pltpu.SMEM(owner_map.shape, owner_map.dtype),
            pltpu.VMEM(dft.shape, dft.dtype),
            pltpu.VMEM(lag.shape, lag.dtype),
            pltpu.VMEM(cos_table.shape, cos_table.dtype),
            pltpu.VMEM(sin_table.shape, sin_table.dtype),
            dma((7,)),
            pltpu.VMEM((blocks, CH_DEV + CH_DEV // 2, 2 * CH_DEV), jnp.bfloat16),
            pltpu.VMEM((CH_DEV, 4 * CH_DEV), jnp.float32),
            pltpu.VMEM((width, 4 * NF), jnp.float32),
            pltpu.VMEM((width + 2 * CH_DEV, 4 * NF), jnp.bfloat16),
            pltpu.VMEM(((blocks + 1) * step_rows, 2 * NF), jnp.float32),
            pltpu.VMEM((blocks + 1, step_rows, 2 * NF), jnp.bfloat16),
            pltpu.VMEM((2, count, step_rows, 2 * NF), jnp.bfloat16),
            pltpu.VMEM((step_rows, 2 * NF), jnp.float32),
            pltpu.VMEM((periods, step_rows, 2 * NF), jnp.bfloat16),
            dma((count,)),
            dma((blocks,)),
            dma,
            dma,
            dma((2 * (blocks + 1),)),
            dma((2, count)),
            dma((periods,)),
            dma((periods,)),
        ],
        compiler_params=pltpu.CompilerParams(collective_id=0, has_side_effects=True),
    )(raw_strain[0], bin_ids, owner_map, dft, lag, cos_table, sin_table)
    return stacked.reshape(2 * MB_DEV, NP, WIN)


def device_shards(mesh, raw_strain, bin_ids, owner_map):
    count, periods = mesh.shape["chan"], mesh.shape["period"]
    whole_windows = raw_strain.shape[1] == WIN and count >= 4 and count & (count - 1) == 0
    if whole_windows and periods % 2 == 0:
        return window_shards(count, periods, raw_strain, bin_ids, owner_map)
    return shards(raw_strain, bin_ids, owner_map)


def solution(mesh):
    placed = (P("period", "chan", None), P(None, "chan", None), P())
    return jax.shard_map(
        functools.partial(device_shards, mesh),
        mesh=mesh,
        in_specs=placed,
        out_specs=P("chan", None, None),
        check_vma=False,
    )
```
